32 devices in a mesh: ep: 8 (over z, y), dp: 4 (over x, core).
Axes of the slice: x: 2, y: 2, z: 4, core: 2. Of those that a mesh axis runs over, the one named last changes fastest.
Arguments:
- tokens: bfloat16 [4096, 2048], P(('dp', 'ep')), parts along dimension 0, may hold values from -6 to 6
- expert_ids: int32 [4096, 2], P(('dp', 'ep')), parts along dimension 0, may hold values from 0 to 7, all different within a row; in each aligned block of 128 rows (0 to 127, 128 to 255, ...) at most 48 rows name the same one
- gate_values: float32 [4096, 2], P(('dp', 'ep')), parts along dimension 0, may hold values from 0.1 to 1
- latent_down: bfloat16 [2048, 512], P('ep'), may hold values from -0.125 to 0.125
- latent_up: bfloat16 [512, 2048], P(None, 'ep'), may hold values from -0.25 to 0.25
- expert_up: bfloat16 [8, 512, 1408], P('ep'), may hold values from -0.25 to 0.25
- expert_down: bfloat16 [8, 1408, 512], P('ep'), may hold values from -0.15625 to 0.15625
- grad_out: bfloat16 [4096, 2048], P(('dp', 'ep')), parts along dimension 0, may hold values from -6 to 6
Outputs:
- layer_out: bfloat16 [4096, 2048], P(('dp', 'ep')), parts along dimension 0
- grad_tokens: bfloat16 [4096, 2048], P(('dp', 'ep')), parts along dimension 0
The draws below stay inside these ranges and needn't reach their ends.
There are 4 independent parts, one for each index of `dp`. The reference program is written for one: setup_inputs(seed, part) draws one part's arguments, and reference() takes and returns one part's arrays. A program takes and returns all parts, laid end to end along the dimension named above; an argument that names none is the same for every part. Nothing has to cross between parts.
Inputs may be any that keep to these rules, and one draw needn't show every extreme that they name: `expert_ids`: each row names 2 different experts. Among the 128 tokens of one device, no expert is named by more than 48 tokens, and in every draw some expert is named by exactly 48 tokens of some device.
All inputs are finite; a program needn't handle non-finite values.
Results may differ from the reference program's by a relative error of at most 0.013.
Values may be sent and summed in bfloat16 or wider, within the bound.
A program may use at most 64 MiB of HBM per device.

```python
import math
import jax
import jax.numpy as jnp
import numpy as np
from jax import lax

D = 2048
L = 512
FF = 1408
TOK_DEV = 128
EXPERTS = 8
TOPK = 2
MOST = 48
TOKENS = 1024
N_EP = 8


def shard_levels(key, shape, split, low, top_value):
    factor_of, own = 1.0, jax.random.fold_in(key, 6)
    for axis_at, parts in split:
        heights = jnp.exp(jax.random.uniform(jax.random.fold_in(own, axis_at), (parts,), jnp.float32, low / len(split), top_value / len(split)))
        factor_of = factor_of * jnp.repeat(heights, shape[axis_at] // parts).reshape([-1 if axis == axis_at else 1 for axis in range(len(shape))])
    return factor_of


def routed_block(own_key, own, number, rows, number_of, top, reach, skew):
    order = jax.random.permutation(own_key, number_of)
    crowded, ordinary = portions_of(number_of, rows * top, reach, skew, True), portions_of(number_of, rows * top, reach, skew, False)
    places = jnp.arange(number_of)

    def named(sizes, turn):
        used = int((sizes > 0).sum())
        fixed = max(1, used // 4)
        shifted = fixed + (places - fixed + turn * (used - fixed)) % max(1, number_of - fixed)
        return jnp.zeros((number_of,), jnp.int32).at[order[jnp.where(places < fixed, places, shifted)]].set(jnp.asarray(sizes, jnp.int32))

    sizes = jnp.where(number % 4 == 0, named(crowded, number // 4), named(ordinary, number - number // 4 - 1))
    mixed = jax.random.permutation(jax.random.fold_in(own, 3), number_of)
    giver, receiver = mixed[0:number_of // 2 * 2:2], mixed[1:number_of // 2 * 2:2]
    slack = jnp.minimum(sizes[giver] - 1, reach - sizes[receiver]) // 2
    slack = jnp.where((giver == order[0]) | (receiver == order[0]) | (sizes[receiver] == 0), 0, jnp.maximum(slack, 0))
    shifted = jax.random.randint(jax.random.fold_in(own, 4), (number_of // 2,), 0, 1 << 20) % (slack + 1)
    sizes = sizes.at[giver].add(-shifted).at[receiver].add(shifted)
    labels = jnp.searchsorted(jnp.cumsum(sizes), jnp.arange(rows * top), side="right").astype(jnp.int32)
    grid = labels.reshape(top, rows).T
    grid = grid[jax.random.permutation(jax.random.fold_in(own, 1), rows)]
    turn = jax.random.randint(jax.random.fold_in(own, 2), (rows, 1), 0, top)
    return jnp.take_along_axis(grid, (jnp.arange(top)[None, :] + turn) % top, axis=1)


def portions_of(amount, total, reach, slope, full):
    loads = [(1 << 20) // math.isqrt(rank ** slope) + 1 for rank in range(1, amount + 1)]
    largest = reach if full else min(reach, max(-(-total // amount), total * loads[0] // sum(loads)))
    least = 1 if total - largest >= amount - 1 else 0
    counts, spare = [largest] + [least] * (amount - 1), total - largest - least * (amount - 1)
    while spare > 0:
        candidates = [i for i in range(1, amount) if counts[i] < largest] or [i for i in range(1, amount) if counts[i] < reach]
        whole, remaining = sum([loads[i] for i in candidates]), spare
        for i in candidates:
            addition = min(reach - counts[i], max(1, remaining * loads[i] // whole), spare)
            counts[i] = counts[i] + addition
            spare = spare - addition
    return np.array(counts)


def gaussian(stream_key, shape, width, bound, split=(), dtype=jnp.bfloat16):
    drawn = jax.random.normal(stream_key, shape, jnp.float32) * width
    if len(split) > 0:
        drawn = shard_levels(stream_key, shape, split, -0.22, 0.18) * drawn
    return jnp.clip(drawn, min=-bound, max=bound).astype(dtype)


def setup_inputs(seed: int = 0, part: int = 0) -> dict:
    seeds = jax.random.split(jax.random.key(seed), 9)
    part_splits = jax.random.split(jax.random.fold_in(seeds[8], part), 9)
    tokens = gaussian(part_splits[0], (TOKENS, D), 1.0, 6.0, ((0, 8),))
    expert_ids_keys = jax.random.split(jax.random.fold_in(part_splits[1], 1), TOKENS // TOK_DEV)
    expert_ids_turns = jax.random.permutation(jax.random.fold_in(part_splits[1], 3), TOKENS // TOK_DEV)
    expert_ids = jax.vmap(lambda own, number: routed_block(jax.random.fold_in(part_splits[1], 2), own, number, TOK_DEV, EXPERTS, TOPK, MOST, 2))(expert_ids_keys, expert_ids_turns).reshape((TOKENS, TOPK))
    gate_values = jnp.clip(jnp.exp(math.log(1.0) - 2.3025851 * jax.random.uniform(part_splits[2], (TOKENS, TOPK), jnp.float32) ** shard_levels(part_splits[2], (TOKENS, TOPK), ((0, 8),), -0.2, 0.2)), 0.1, 1.0)
    latent_down = gaussian(seeds[3], (D, L), D ** -0.5, 0.125, ((0, 8),))
    latent_up = gaussian(seeds[4], (L, D), L ** -0.5, 0.25, ((1, 8),))
    expert_up = gaussian(seeds[5], (EXPERTS, L, FF), L ** -0.5, 0.25, ((0, 8),))
    expert_down = gaussian(seeds[6], (EXPERTS, FF, L), FF ** -0.5, 0.15625, ((0, 8),))
    grad_out = gaussian(part_splits[7], (TOKENS, D), 1.0, 6.0, ((0, 8),))
    return dict(tokens=tokens, expert_ids=expert_ids, gate_values=gate_values, latent_down=latent_down, latent_up=latent_up, expert_up=expert_up, expert_down=expert_down, grad_out=grad_out)


def contract_last(left, right):
    return lax.dot_general(left, right, (((1,), (1,)), ((), ())), preferred_element_type=jnp.float32)


def reference(tokens, expert_ids, gate_values, latent_down, latent_up, expert_up, expert_down, grad_out):
    latent = jnp.dot(tokens, latent_down, preferred_element_type=jnp.float32).astype(jnp.bfloat16)
    grad_latent = contract_last(grad_out, latent_up)
    capacity = N_EP * MOST
    flat_ids = expert_ids.reshape(-1)
    flat_tok = (jnp.arange(flat_ids.shape[0]) // TOPK).astype(jnp.int32)
    flat_gate = gate_values.reshape(-1)
    numbers = jnp.arange(EXPERTS).astype(jnp.int32)
    row_count = tokens.shape[0]

    def per_expert(totals, inputs):
        combined, grad_sum = totals
        expert_num, up_weight, down_weight = inputs
        member = flat_ids == expert_num
        filled = jnp.sum(member.astype(jnp.int32))
        chosen = jnp.nonzero(member, size=capacity, fill_value=0)[0].astype(jnp.int32)
        live_slot = jnp.arange(capacity) < filled
        token_rows = flat_tok[chosen]
        gate_col = jnp.where(live_slot, flat_gate[chosen], jnp.zeros_like(flat_gate[chosen]))[:, None]
        arrived = latent[token_rows]
        pre_act = jnp.dot(arrived, up_weight, preferred_element_type=jnp.float32)
        squared = jnp.square(jax.nn.relu(pre_act)).astype(jnp.bfloat16)
        expert_out = jnp.dot(squared, down_weight, preferred_element_type=jnp.float32).astype(jnp.bfloat16)
        combined = combined.at[token_rows].add(gate_col * expert_out.astype(jnp.float32))
        grad_rows = (gate_col * grad_latent[token_rows]).astype(jnp.bfloat16)
        grad_act = contract_last(grad_rows, down_weight)
        grad_pre = (2.0 * jax.nn.relu(pre_act) * grad_act).astype(jnp.bfloat16)
        grad_in = contract_last(grad_pre, up_weight).astype(jnp.bfloat16).astype(jnp.float32)
        grad_in = jnp.where(live_slot[:, None], grad_in, jnp.zeros_like(grad_in))
        grad_sum = grad_sum.at[token_rows].add(grad_in)
        return (combined, grad_sum), None

    start_totals = (jnp.zeros((row_count, L), jnp.float32), jnp.zeros((row_count, L), jnp.float32))
    (combined, grad_sum), unused = lax.scan(per_expert, start_totals, (numbers, expert_up, expert_down))
    layer_out = jnp.dot(combined.astype(jnp.bfloat16), latent_up, preferred_element_type=jnp.float32).astype(jnp.bfloat16)
    grad_tokens = contract_last(grad_sum.astype(jnp.bfloat16), latent_down).astype(jnp.bfloat16)
    return (layer_out, grad_tokens)
```

```python
import functools

import jax
import jax.numpy as jnp
from jax import lax
from jax.experimental import pallas as pl
from jax.experimental.pallas import tpu as pltpu
from jax.sharding import PartitionSpec as P

MESH = pl.DeviceIdType.MESH
ROW_TILE = 16

DOWN, UP, LATENT, GRAD, FORWARD, BACKWARD, DOWN_TWIN, UP_TWIN = range(8)


def dot(left, right):
    return jnp.dot(left, right, preferred_element_type=jnp.float32)


def contract_last(left, right):
    return lax.dot_general(
        left, right, (((1,), (1,)), ((), ())), preferred_element_type=jnp.float32
    )


def kernel(
    ep_size,
    share,
    slots,
    ids_ref,
    gates_ref,
    tokens_hbm,
    grad_out_hbm,
    down_hbm,
    up_hbm,
    expert_up_hbm,
    expert_down_hbm,
    layer_ref,
    grad_ref,
    tokens,
    grad_out,
    expert_up,
    expert_down,
    full_down,
    full_up,
    lat_send,
    lat_recv,
    grad_send,
    grad_recv,
    pre_act,
    out_send,
    out_recv,
    in_send,
    in_recv,
    local_sem,
    send_sem,
    recv_sem,
):
    me = lax.axis_index("ep")
    row = lax.axis_index("dp")
    twin = row + 1 - 2 * lax.rem(row, 2)
    part = lax.rem(row, 2) if share == 2 else 0
    other = 1 - part
    shard = down_hbm.shape[0]
    piece = shard // share
    tok_rows = tokens.shape[0]
    total = lat_send.shape[0]
    bf16 = jnp.bfloat16

    def peers(body):
        lax.fori_loop(1, ep_size, lambda d, c: (body(d), c)[1], 0)

    def after(d):
        return lax.rem(me + d, ep_size)

    def ahead(d):
        return lax.rem(me + ep_size - d, ep_size)

    loads = [
        pltpu.make_async_copy(src, dst, local_sem.at[i])
        for i, (src, dst) in enumerate(
            (
                (tokens_hbm, tokens),
                (grad_out_hbm, grad_out),
                (expert_up_hbm.at[0], expert_up),
                (expert_down_hbm.at[0], expert_down),
                (down_hbm, full_down.at[pl.ds(pl.multiple_of(me * shard, ROW_TILE), shard)]),
                (up_hbm, full_up.at[pl.ds(pl.multiple_of(me * shard, ROW_TILE), shard)]),
            )
        )
    ]
    for load in loads:
        load.start()

    barrier = pltpu.get_barrier_semaphore()

    def greet(d):
        pl.semaphore_signal(barrier, inc=1, device_id={"ep": after(d)}, device_id_type=MESH)

    peers(greet)
    if share == 2:
        pl.semaphore_signal(barrier, inc=1, device_id={"dp": twin}, device_id_type=MESH)
    pl.semaphore_wait(barrier, ep_size - 1 + (share - 1))

    def piece_at(owner, which):
        return pl.ds(pl.multiple_of(owner * shard + which * piece, ROW_TILE), piece)

    def gather_copy(kind, src, full, owner, peer):
        return pltpu.make_async_remote_copy(
            src_ref=src.at[pl.ds(pl.multiple_of(part * piece, ROW_TILE), piece)],
            dst_ref=full.at[piece_at(owner, part)],
            send_sem=send_sem.at[kind, peer],
            recv_sem=recv_sem.at[kind, owner],
            device_id={"ep": peer},
            device_id_type=MESH,
        )

    def twin_copy(kind, full, owner, which):
        return pltpu.make_async_remote_copy(
            src_ref=full.at[piece_at(owner, which)],
            dst_ref=full.at[piece_at(owner, which)],
            send_sem=send_sem.at[kind, owner],
            recv_sem=recv_sem.at[kind, owner],
            device_id={"dp": twin},
            device_id_type=MESH,
        )

    peers(lambda d: gather_copy(DOWN, down_hbm, full_down, me, after(d)).start())
    peers(lambda d: gather_copy(UP, up_hbm, full_up, me, after(d)).start())

    def slot_at(index):
        return pl.ds(pl.multiple_of(index * slots, ROW_TILE), slots)

    def exchange_copy(kind, send, recv, peer, owner):
        return pltpu.make_async_remote_copy(
            src_ref=send.at[slot_at(peer)],
            dst_ref=recv.at[slot_at(owner)],
            send_sem=send_sem.at[kind, peer],
            recv_sem=recv_sem.at[kind, owner],
            device_id={"ep": peer},
            device_id_type=MESH,
        )

    def own_copy(kind, send, recv):
        return pltpu.make_async_copy(
            send.at[slot_at(me)], recv.at[slot_at(me)], recv_sem.at[kind, me]
        )

    def exchange_start(kind, send, recv):
        peers(lambda d: exchange_copy(kind, send, recv, after(d), me).start())
        own_copy(kind, send, recv).start()

    def exchange_wait(kind, send, recv):
        own_copy(kind, send, recv).wait()
        peers(lambda d: exchange_copy(kind, send, recv, after(d), ahead(d)).wait_recv())

    ids = ids_ref[...]
    gates = gates_ref[...]
    choices = ids.shape[1]
    lanes = lax.broadcasted_iota(jnp.int32, (tok_rows, ep_size), 1)
    picks = [(ids[:, k : k + 1] == lanes).astype(jnp.float32) for k in range(choices)]
    routed = functools.reduce(jnp.add, picks)
    lower = (
        lax.broadcasted_iota(jnp.int32, (tok_rows, tok_rows), 1)
        < lax.broadcasted_iota(jnp.int32, (tok_rows, tok_rows), 0)
    ).astype(bf16)
    before = dot(lower, routed.astype(bf16))
    by_token = lax.broadcasted_iota(jnp.int32, (tok_rows, total), 1)
    by_slot = lax.broadcasted_iota(jnp.int32, (total, tok_rows), 0)
    take, place = [], []
    for k in range(choices):
        pos = jnp.sum(picks[k] * before, axis=1, keepdims=True)
        flat = ids[:, k : k + 1].astype(jnp.float32) * slots + pos
        take.append((flat.astype(jnp.int32) == by_token).astype(bf16))
        flat_row = jnp.transpose(jnp.broadcast_to(flat, (tok_rows, tok_rows)))[0:1, :]
        place.append((flat_row.astype(jnp.int32) == by_slot).astype(bf16))

    def gather_wait(kind, twin_kind, src, full, first, last):
        def arrive(d, c):
            gather_copy(kind, src, full, ahead(d), after(d)).wait_recv()
            if share == 2:
                twin_copy(twin_kind, full, ahead(d), part).start()
            return c

        lax.fori_loop(first, last, arrive, 0)

    def twin_wait(twin_kind, full):
        if share == 2:
            peers(lambda d: twin_copy(twin_kind, full, ahead(d), other).wait_recv())

    gather_wait(DOWN, DOWN_TWIN, down_hbm, full_down, 1, ep_size)
    loads[0].wait()
    loads[4].wait()
    twin_wait(DOWN_TWIN, full_down)
    latent = dot(tokens[...], full_down[...]).astype(bf16)
    lat_send[...] = dot(functools.reduce(jnp.add, place), latent).astype(bf16)
    exchange_start(LATENT, lat_send, lat_recv)

    middle = 1 + ep_size // 2
    gather_wait(UP, UP_TWIN, up_hbm, full_up, 1, middle)

    rows = total if total <= 512 else 256
    blocks = total // rows

    def each_block(body):
        if blocks == 1:
            body(slice(None))
        else:
            lax.fori_loop(
                0,
                blocks,
                lambda b, c: (body(pl.ds(pl.multiple_of(b * rows, ROW_TILE), rows)), c)[1],
                0,
            )

    def forward(at):
        hidden = jnp.maximum(dot(lat_recv[at, :], expert_up[...]), 0.0)
        pre_act[at, :] = hidden
        out_send[at, :] = dot((hidden * hidden).astype(bf16), expert_down[...]).astype(bf16)

    loads[2].wait()
    loads[3].wait()
    exchange_wait(LATENT, lat_send, lat_recv)
    each_block(forward)
    exchange_start(FORWARD, out_send, out_recv)

    gather_wait(UP, UP_TWIN, up_hbm, full_up, middle, ep_size)
    loads[1].wait()
    loads[5].wait()
    twin_wait(UP_TWIN, full_up)
    grad_latent = dot(grad_out[...], full_up[...])
    sent = [
        dot(place[k], (gates[:, k : k + 1] * grad_latent).astype(bf16)) for k in range(choices)
    ]
    grad_send[...] = functools.reduce(jnp.add, sent).astype(bf16)
    exchange_start(GRAD, grad_send, grad_recv)

    exchange_wait(FORWARD, out_send, out_recv)
    returned = out_recv[...]
    combined = functools.reduce(
        jnp.add, [gates[:, k : k + 1] * dot(take[k], returned) for k in range(choices)]
    ).astype(bf16)
    layer_ref[...] = contract_last(combined, full_up[...]).astype(bf16)

    def backward(at):
        grad_act = contract_last(grad_recv[at, :], expert_down[...])
        grad_pre = (2.0 * pre_act[at, :] * grad_act).astype(bf16)
        in_send[at, :] = contract_last(grad_pre, expert_up[...]).astype(bf16)

    exchange_wait(GRAD, grad_send, grad_recv)
    each_block(backward)
    exchange_start(BACKWARD, in_send, in_recv)
    exchange_wait(BACKWARD, in_send, in_recv)
    grad_sum = dot(functools.reduce(jnp.add, take), in_recv[...]).astype(bf16)
    grad_ref[...] = contract_last(grad_sum, full_down[...]).astype(bf16)

    def finish(d):
        gather_copy(DOWN, down_hbm, full_down, me, after(d)).wait_send()
        gather_copy(UP, up_hbm, full_up, me, after(d)).wait_send()
        exchange_copy(LATENT, lat_send, lat_recv, after(d), me).wait_send()
        exchange_copy(GRAD, grad_send, grad_recv, after(d), me).wait_send()
        exchange_copy(FORWARD, out_send, out_recv, after(d), me).wait_send()
        exchange_copy(BACKWARD, in_send, in_recv, after(d), me).wait_send()
        if share == 2:
            twin_copy(DOWN_TWIN, full_down, after(d), part).wait_send()
            twin_copy(UP_TWIN, full_up, after(d), part).wait_send()

    peers(finish)


def on_device(
    tokens, expert_ids, gate_values, latent_down, latent_up, expert_up, expert_down, grad_out
):
    ep_size = lax.axis_size("ep")
    dp_size = lax.axis_size("dp")
    tok_rows, model = tokens.shape
    top_count = expert_ids.shape[1]
    local_experts, width, hidden = expert_up.shape
    assert local_experts == 1
    experts = local_experts * ep_size
    capacity = max(2, (3 * tok_rows * top_count + 2 * experts - 1) // (2 * experts))
    slots = (capacity + ROW_TILE - 1) // ROW_TILE * ROW_TILE
    total = experts * slots
    shard = latent_down.shape[0]
    share = 2 if dp_size % 2 == 0 and shard % (2 * ROW_TILE) == 0 else 1
    bf16 = jnp.bfloat16
    buffer = pltpu.VMEM((total, width), bf16)
    vmem = pl.BlockSpec(memory_space=pltpu.VMEM)
    anywhere = pl.BlockSpec(memory_space=pl.ANY)
    return pl.pallas_call(
        functools.partial(kernel, ep_size, share, slots),
        out_shape=[jax.ShapeDtypeStruct((tok_rows, model), bf16)] * 2,
        in_specs=[vmem, vmem] + [anywhere] * 6,
        out_specs=[vmem, vmem],
        scratch_shapes=[
            pltpu.VMEM((tok_rows, model), bf16),
            pltpu.VMEM((tok_rows, model), bf16),
            pltpu.VMEM((width, hidden), bf16),
            pltpu.VMEM((hidden, width), bf16),
            pltpu.VMEM((model, width), bf16),
            pltpu.VMEM((model, width), bf16),
            buffer,
            buffer,
            buffer,
            buffer,
            pltpu.VMEM((total, hidden), jnp.float32),
            buffer,
            buffer,
            buffer,
            buffer,
            pltpu.SemaphoreType.DMA((6,)),
            pltpu.SemaphoreType.DMA((8, ep_size)),
            pltpu.SemaphoreType.DMA((8, ep_size)),
        ],
        compiler_params=pltpu.CompilerParams(
            collective_id=0, has_side_effects=True, vmem_limit_bytes=60 * 1024 * 1024
        ),
    )(
        expert_ids,
        gate_values,
        tokens,
        grad_out,
        latent_down,
        latent_up.T,
        expert_up,
        expert_down,
    )


def solution(mesh):
    placed = (
        P(("dp", "ep"), None),
        P(("dp", "ep"), None),
        P(("dp", "ep"), None),
        P("ep", None),
        P(None, "ep"),
        P("ep", None, None),
        P("ep", None, None),
        P(("dp", "ep"), None),
    )
    return jax.shard_map(
        on_device,
        mesh=mesh,
        in_specs=placed,
        out_specs=(P(("dp", "ep"), None), P(("dp", "ep"), None)),
        check_vma=False,
    )
```

```python
import functools

import jax
import jax.numpy as jnp
from jax import lax
from jax.experimental import pallas as pl
from jax.experimental.pallas import tpu as pltpu
from jax.sharding import PartitionSpec as P

MESH = pl.DeviceIdType.MESH
ROW_TILE = 16

UPWARD, DOWNWARD, ACROSS, TWIN = range(4)
LATENT, GRAD, FORWARD, BACKWARD = range(4)
SEND_BASE, RECV_BASE = 8, 4


def dot(left, right):
    return jnp.dot(left, right, preferred_element_type=jnp.float32)


def contract_last(left, right):
    return lax.dot_general(
        left, right, (((1,), (1,)), ((), ())), preferred_element_type=jnp.float32
    )


def kernel(
    ep_size,
    share,
    slots,
    ids_ref,
    gates_ref,
    tokens_hbm,
    grad_out_hbm,
    down_hbm,
    up_hbm,
    expert_up_hbm,
    expert_down_hbm,
    layer_ref,
    grad_ref,
    tokens,
    grad_out,
    expert_up,
    expert_down,
    full_down,
    full_up,
    up_shard,
    lat_send,
    lat_recv,
    grad_send,
    grad_recv,
    pre_act,
    out_send,
    out_recv,
    in_send,
    in_recv,
    local_sem,
    send_sem,
    recv_sem,
):
    me = lax.axis_index("ep")
    row = lax.axis_index("dp")
    twin = row + 1 - 2 * lax.rem(row, 2)
    part = lax.rem(row, 2) if share == 2 else 0
    other = 1 - part
    shard = down_hbm.shape[0]
    piece = shard // share
    tok_rows = tokens.shape[0]
    total = lat_send.shape[0]
    bf16 = jnp.bfloat16

    def peers(body):
        lax.fori_loop(1, ep_size, lambda d, c: (body(d), c)[1], 0)

    def after(d):
        return lax.rem(me + d, ep_size)

    def ahead(d):
        return lax.rem(me + ep_size - d, ep_size)

    loads = [
        pltpu.make_async_copy(src, dst, local_sem.at[i])
        for i, (src, dst) in enumerate(
            (
                (tokens_hbm, tokens),
                (grad_out_hbm, grad_out),
                (expert_up_hbm.at[0], expert_up),
                (expert_down_hbm.at[0], expert_down),
                (down_hbm, full_down.at[pl.ds(pl.multiple_of(me * shard, ROW_TILE), shard)]),
                (up_hbm, up_shard),
            )
        )
    ]
    for load in loads:
        load.start()

    barrier = pltpu.get_barrier_semaphore()

    def greet(d):
        pl.semaphore_signal(barrier, inc=1, device_id={"ep": after(d)}, device_id_type=MESH)

    peers(greet)
    if share == 2:
        pl.semaphore_signal(barrier, inc=1, device_id={"dp": twin}, device_id_type=MESH)
    pl.semaphore_wait(barrier, ep_size - 1 + (share - 1))

    def piece_at(owner, which):
        return pl.ds(pl.multiple_of(owner * shard + which * piece, ROW_TILE), piece)

    full = (full_down, full_up)
    height = ep_size // 2
    level = me // 2
    side = lax.rem(me, 2)

    def piece_copy(m, owner, which, target, row_of, from_twin=0):
        return pltpu.make_async_remote_copy(
            src_ref=full[m].at[piece_at(owner, which)],
            dst_ref=full[m].at[piece_at(owner, which)],
            send_sem=send_sem.at[4 * m + row_of, owner],
            recv_sem=recv_sem.at[2 * m + from_twin, owner],
            device_id=target,
            device_id_type=MESH,
        )

    def upward(m, owner):
        return piece_copy(m, owner, part, {"ep": me + 2}, UPWARD)

    def downward(m, owner):
        return piece_copy(m, owner, part, {"ep": me - 2}, DOWNWARD)

    def across(m, owner):
        return piece_copy(m, owner, part, {"ep": me + 1 - 2 * side}, ACROSS)

    def to_twin(m, owner, which):
        return piece_copy(m, owner, which, {"dp": twin}, TWIN, 1)

    def own_each(m, act):
        @pl.when(level + 1 < height)
        def _():
            act(upward(m, me))

        @pl.when(level > 0)
        def _():
            act(downward(m, me))

        act(across(m, me))

    def relay_each(m, d, act, arrive):
        @pl.when(level >= d)
        def _():
            owner = me - 2 * d
            arrive(m, owner)

            @pl.when(level + 1 < height)
            def _():
                act(upward(m, owner))

            act(across(m, owner))
            if share == 2:
                act(to_twin(m, owner, part))

        @pl.when(level + d < height)
        def _():
            owner = me + 2 * d
            arrive(m, owner)

            @pl.when(level > 0)
            def _():
                act(downward(m, owner))

            act(across(m, owner))
            if share == 2:
                act(to_twin(m, owner, part))

    def cross_each(m, d, act, arrive):
        partner = me + 1 - 2 * side

        @pl.when(level >= d)
        def _():
            arrive(m, partner - 2 * d)
            if share == 2:
                act(to_twin(m, partner - 2 * d, part))

        if not (isinstance(d, int) and d == 0):

            @pl.when(level + d < height)
            def _():
                arrive(m, partner + 2 * d)
                if share == 2:
                    act(to_twin(m, partner + 2 * d, part))

    def begin(copy):
        copy.start()

    def arrived(m, owner):
        across(m, owner).wait_recv()

    def steps(m, first, last):
        def body(d, c):
            relay_each(m, d, begin, arrived)

            @pl.when(d > 1)
            def _():
                cross_each(m, d - 1, begin, arrived)

            return c

        lax.fori_loop(first, last, body, 0)

    def gather_end(m):
        if height > 1:
            cross_each(m, height - 1, begin, arrived)
        if share == 2:
            peers(lambda d: to_twin(m, ahead(d), other).wait_recv())

    loads[4].wait()
    own_each(0, begin)

    def slot_at(index):
        return pl.ds(pl.multiple_of(index * slots, ROW_TILE), slots)

    def exchange_copy(kind, send, recv, peer, owner):
        return pltpu.make_async_remote_copy(
            src_ref=send.at[slot_at(peer)],
            dst_ref=recv.at[slot_at(owner)],
            send_sem=send_sem.at[SEND_BASE + kind, peer],
            recv_sem=recv_sem.at[RECV_BASE + kind, owner],
            device_id={"ep": peer},
            device_id_type=MESH,
        )

    def own_copy(kind, send, recv):
        return pltpu.make_async_copy(
            send.at[slot_at(me)], recv.at[slot_at(me)], recv_sem.at[RECV_BASE + kind, me]
        )

    def exchange_start(kind, send, recv):
        peers(lambda d: exchange_copy(kind, send, recv, after(d), me).start())
        own_copy(kind, send, recv).start()

    def exchange_wait(kind, send, recv):
        own_copy(kind, send, recv).wait()
        peers(lambda d: exchange_copy(kind, send, recv, after(d), ahead(d)).wait_recv())

    choices = ids_ref.shape[0]

    def as_column(line):
        return jnp.transpose(jnp.broadcast_to(line, (tok_rows, tok_rows)))[:, 0:1]

    ids = [
        as_column(ids_ref[k : k + 1, :].astype(jnp.float32)).astype(jnp.int32)
        for k in range(choices)
    ]
    gates = [as_column(gates_ref[k : k + 1, :]) for k in range(choices)]
    lanes = lax.broadcasted_iota(jnp.int32, (tok_rows, ep_size), 1)
    picks = [(ids[k] == lanes).astype(jnp.float32) for k in range(choices)]
    routed = functools.reduce(jnp.add, picks)
    lower = (
        lax.broadcasted_iota(jnp.int32, (tok_rows, tok_rows), 1)
        < lax.broadcasted_iota(jnp.int32, (tok_rows, tok_rows), 0)
    ).astype(bf16)
    before = dot(lower, routed.astype(bf16))
    by_token = lax.broadcasted_iota(jnp.int32, (tok_rows, total), 1)
    by_slot = lax.broadcasted_iota(jnp.int32, (total, tok_rows), 0)
    take, place = [], []
    for k in range(choices):
        pos = jnp.sum(picks[k] * before, axis=1, keepdims=True)
        flat = ids[k].astype(jnp.float32) * slots + pos
        take.append((flat.astype(jnp.int32) == by_token).astype(bf16))
        flat_row = jnp.transpose(jnp.broadcast_to(flat, (tok_rows, tok_rows)))[0:1, :]
        place.append((flat_row.astype(jnp.int32) == by_slot).astype(bf16))

    loads[5].wait()
    full_up[pl.ds(pl.multiple_of(me * shard, ROW_TILE), shard), :] = jnp.transpose(
        up_shard[...].astype(jnp.float32)
    ).astype(bf16)

    steps(0, 1, 2)
    cross_each(0, 0, begin, arrived)
    own_each(1, begin)
    steps(0, 2, height)
    steps(1, 1, 2)
    cross_each(1, 0, begin, arrived)
    gather_end(0)
    loads[0].wait()
    latent = dot(tokens[...], full_down[...]).astype(bf16)
    lat_send[...] = dot(functools.reduce(jnp.add, place), latent).astype(bf16)
    exchange_start(LATENT, lat_send, lat_recv)

    steps(1, 2, height)
    gather_end(1)
    loads[1].wait()
    grad_latent = dot(grad_out[...], full_up[...])
    sent = [dot(place[k], (gates[k] * grad_latent).astype(bf16)) for k in range(choices)]
    grad_send[...] = functools.reduce(jnp.add, sent).astype(bf16)
    exchange_start(GRAD, grad_send, grad_recv)

    rows = total if total <= 512 else 256
    blocks = total // rows

    def each_block(body):
        if blocks == 1:
            body(slice(None))
        else:
            lax.fori_loop(
                0,
                blocks,
                lambda b, c: (body(pl.ds(pl.multiple_of(b * rows, ROW_TILE), rows)), c)[1],
                0,
            )

    def forward(at):
        hidden = jnp.maximum(dot(lat_recv[at, :], expert_up[...]), 0.0)
        pre_act[at, :] = hidden
        out_send[at, :] = dot((hidden * hidden).astype(bf16), expert_down[...]).astype(bf16)

    loads[2].wait()
    loads[3].wait()
    exchange_wait(LATENT, lat_send, lat_recv)
    each_block(forward)
    exchange_start(FORWARD, out_send, out_recv)

    def backward(at):
        grad_act = contract_last(grad_recv[at, :], expert_down[...])
        grad_pre = (2.0 * pre_act[at, :] * grad_act).astype(bf16)
        in_send[at, :] = contract_last(grad_pre, expert_up[...]).astype(bf16)

    exchange_wait(GRAD, grad_send, grad_recv)
    each_block(backward)
    exchange_start(BACKWARD, in_send, in_recv)

    exchange_wait(FORWARD, out_send, out_recv)
    returned = out_recv[...]
    combined = functools.reduce(
        jnp.add, [gates[k] * dot(take[k], returned) for k in range(choices)]
    ).astype(bf16)
    layer_ref[...] = contract_last(combined, full_up[...]).astype(bf16)

    exchange_wait(BACKWARD, in_send, in_recv)
    grad_sum = dot(functools.reduce(jnp.add, take), in_recv[...]).astype(bf16)
    grad_ref[...] = contract_last(grad_sum, full_down[...]).astype(bf16)

    def finish(d):
        exchange_copy(LATENT, lat_send, lat_recv, after(d), me).wait_send()
        exchange_copy(GRAD, grad_send, grad_recv, after(d), me).wait_send()
        exchange_copy(FORWARD, out_send, out_recv, after(d), me).wait_send()
        exchange_copy(BACKWARD, in_send, in_recv, after(d), me).wait_send()

    peers(finish)

    def end(copy):
        copy.wait_send()

    def nothing(m, owner):
        del m, owner

    for m in range(2):
        own_each(m, end)
        cross_each(m, 0, end, nothing)

        def drain(d, c, m=m):
            relay_each(m, d, end, nothing)
            cross_each(m, d, end, nothing)
            return c

        lax.fori_loop(1, height, drain, 0)


def on_device(
    tokens, expert_ids, gate_values, latent_down, latent_up, expert_up, expert_down, grad_out
):
    ep_size = lax.axis_size("ep")
    dp_size = lax.axis_size("dp")
    tok_rows, model = tokens.shape
    top_count = expert_ids.shape[1]
    local_experts, width, hidden = expert_up.shape
    assert local_experts == 1 and ep_size % 2 == 0
    experts = local_experts * ep_size
    capacity = max(2, (3 * tok_rows * top_count + 2 * experts - 1) // (2 * experts))
    slots = (capacity + ROW_TILE - 1) // ROW_TILE * ROW_TILE
    total = experts * slots
    shard = latent_down.shape[0]
    share = 2 if dp_size % 2 == 0 and shard % (2 * ROW_TILE) == 0 else 1
    bf16 = jnp.bfloat16
    buffer = pltpu.VMEM((total, width), bf16)
    vmem = pl.BlockSpec(memory_space=pltpu.VMEM)
    anywhere = pl.BlockSpec(memory_space=pl.ANY)
    return pl.pallas_call(
        functools.partial(kernel, ep_size, share, slots),
        out_shape=[jax.ShapeDtypeStruct((tok_rows, model), bf16)] * 2,
        in_specs=[vmem, vmem] + [anywhere] * 6,
        out_specs=[vmem, vmem],
        scratch_shapes=[
            pltpu.VMEM((tok_rows, model), bf16),
            pltpu.VMEM((tok_rows, model), bf16),
            pltpu.VMEM((width, hidden), bf16),
            pltpu.VMEM((hidden, width), bf16),
            pltpu.VMEM((model, width), bf16),
            pltpu.VMEM((model, width), bf16),
            pltpu.VMEM((width, shard), bf16),
            buffer,
            buffer,
            buffer,
            buffer,
            pltpu.VMEM((total, hidden), jnp.float32),
            buffer,
            buffer,
            buffer,
            buffer,
            pltpu.SemaphoreType.DMA((6,)),
            pltpu.SemaphoreType.DMA((12, ep_size)),
            pltpu.SemaphoreType.DMA((8, ep_size)),
        ],
        compiler_params=pltpu.CompilerParams(
            collective_id=0, has_side_effects=True, vmem_limit_bytes=60 * 1024 * 1024
        ),
    )(
        expert_ids.T,
        gate_values.T,
        tokens,
        grad_out,
        latent_down,
        latent_up,
        expert_up,
        expert_down,
    )


def solution(mesh):
    placed = (
        P(("dp", "ep"), None),
        P(("dp", "ep"), None),
        P(("dp", "ep"), None),
        P("ep", None),
        P(None, "ep"),
        P("ep", None, None),
        P("ep", None, None),
        P(("dp", "ep"), None),
    )
    return jax.shard_map(
        on_device,
        mesh=mesh,
        in_specs=placed,
        out_specs=(P(("dp", "ep"), None), P(("dp", "ep"), None)),
        check_vma=False,
    )
```

```python
import functools

import jax
import jax.numpy as jnp
from jax import lax
from jax.experimental import pallas as pl
from jax.experimental.pallas import tpu as pltpu
from jax.sharding import PartitionSpec as P

MESH = pl.DeviceIdType.MESH
ROW_TILE = 16

UPWARD, DOWNWARD, ACROSS, TWIN, MATE, TWIN_MATE = range(6)
LATENT, GRAD, FORWARD, BACKWARD = range(4)
SEND_BASE, RECV_BASE = 12, 8


def dot(left, right):
    return jnp.dot(left, right, preferred_element_type=jnp.float32)


def contract_last(left, right):
    return lax.dot_general(
        left, right, (((1,), (1,)), ((), ())), preferred_element_type=jnp.float32
    )


def kernel(
    ep_size,
    share,
    slots,
    ids_ref,
    gates_ref,
    tokens_hbm,
    grad_out_hbm,
    down_hbm,
    up_hbm,
    expert_up_hbm,
    expert_down_hbm,
    layer_ref,
    grad_ref,
    tokens,
    grad_out,
    expert_up,
    expert_down,
    full_down,
    full_up,
    up_shard,
    lat_send,
    lat_recv,
    grad_send,
    grad_recv,
    pre_act,
    out_send,
    out_recv,
    in_send,
    in_recv,
    local_sem,
    send_sem,
    recv_sem,
):
    me = lax.axis_index("ep")
    row = lax.axis_index("dp")
    twin = row + 1 - 2 * lax.rem(row, 2)
    mate = row + 2 - 4 * lax.rem(row // 2, 2)
    part, twin_part, mate_part = [
        lax.rem(r, 4) if share > 1 else 0 for r in (row, twin, mate)
    ]
    twin_mate_part = 6 - part - twin_part - mate_part
    shard = down_hbm.shape[0]
    piece = shard // share
    tok_rows = tokens.shape[0]
    total = lat_send.shape[0]
    bf16 = jnp.bfloat16

    def peers(body):
        lax.fori_loop(1, ep_size, lambda d, c: (body(d), c)[1], 0)

    def after(d):
        return lax.rem(me + d, ep_size)

    def ahead(d):
        return lax.rem(me + ep_size - d, ep_size)

    loads = [
        pltpu.make_async_copy(src, dst, local_sem.at[i])
        for i, (src, dst) in enumerate(
            (
                (tokens_hbm, tokens),
                (grad_out_hbm, grad_out),
                (expert_up_hbm.at[0], expert_up),
                (expert_down_hbm.at[0], expert_down),
                (down_hbm, full_down.at[pl.ds(pl.multiple_of(me * shard, ROW_TILE), shard)]),
                (up_hbm, up_shard),
            )
        )
    ]
    for load in loads:
        load.start()

    barrier = pltpu.get_barrier_semaphore()

    def greet(d):
        pl.semaphore_signal(barrier, inc=1, device_id={"ep": after(d)}, device_id_type=MESH)

    peers(greet)
    if share > 1:
        pl.semaphore_signal(barrier, inc=1, device_id={"dp": twin}, device_id_type=MESH)
        pl.semaphore_signal(barrier, inc=1, device_id={"dp": mate}, device_id_type=MESH)
    pl.semaphore_wait(barrier, ep_size - 1 + (2 if share > 1 else 0))

    def piece_at(owner, which):
        return pl.ds(pl.multiple_of(owner * shard + which * piece, ROW_TILE), piece)

    full = (full_down, full_up)
    height = ep_size // 2
    level = me // 2
    side = lax.rem(me, 2)

    def piece_copy(m, owner, which, target, row_of, arrival=0):
        return pltpu.make_async_remote_copy(
            src_ref=full[m].at[piece_at(owner, which)],
            dst_ref=full[m].at[piece_at(owner, which)],
            send_sem=send_sem.at[6 * m + row_of, owner],
            recv_sem=recv_sem.at[4 * m + arrival, owner],
            device_id=target,
            device_id_type=MESH,
        )

    def upward(m, owner):
        return piece_copy(m, owner, part, {"ep": me + 2}, UPWARD)

    def downward(m, owner):
        return piece_copy(m, owner, part, {"ep": me - 2}, DOWNWARD)

    def across(m, owner):
        return piece_copy(m, owner, part, {"ep": me + 1 - 2 * side}, ACROSS)

    def to_twin(m, owner, which):
        return piece_copy(m, owner, which, {"dp": twin}, TWIN, 1)

    def to_mate(m, owner, which):
        return piece_copy(m, owner, which, {"dp": mate}, MATE, 2)

    def pass_mate(m, owner, which):
        return piece_copy(m, owner, which, {"dp": twin}, TWIN_MATE, 3)

    def share_out(m, owner, act):
        if share > 1:
            act(to_mate(m, owner, part))
            act(to_twin(m, owner, part))

    def own_each(m, act):
        @pl.when(level + 1 < height)
        def _():
            act(upward(m, me))

        @pl.when(level > 0)
        def _():
            act(downward(m, me))

        act(across(m, me))

    def relay_each(m, d, act, arrive):
        @pl.when(level >= d)
        def _():
            owner = me - 2 * d
            arrive(m, owner)

            @pl.when(level + 1 < height)
            def _():
                act(upward(m, owner))

            act(across(m, owner))
            share_out(m, owner, act)

        @pl.when(level + d < height)
        def _():
            owner = me + 2 * d
            arrive(m, owner)

            @pl.when(level > 0)
            def _():
                act(downward(m, owner))

            act(across(m, owner))
            share_out(m, owner, act)

    def cross_each(m, d, act, arrive):
        partner = me + 1 - 2 * side

        @pl.when(level >= d)
        def _():
            arrive(m, partner - 2 * d)
            share_out(m, partner - 2 * d, act)

        if not (isinstance(d, int) and d == 0):

            @pl.when(level + d < height)
            def _():
                arrive(m, partner + 2 * d)
                share_out(m, partner + 2 * d, act)

    def begin(copy):
        copy.start()

    def arrived(m, owner):
        across(m, owner).wait_recv()

    def steps(m, first, last):
        def body(d, c):
            relay_each(m, d, begin, arrived)

            @pl.when(d > 1)
            def _():
                cross_each(m, d - 1, begin, arrived)

            return c

        lax.fori_loop(first, last, body, 0)

    def gather_end(m):
        if height > 1:
            cross_each(m, height - 1, begin, arrived)
        if share > 1:

            def pass_on(level_of, side_of):
                owner = level_of * 2 + side_of
                to_mate(m, owner, mate_part).wait_recv()
                pass_mate(m, owner, mate_part).start()

            def near(d, c):
                @pl.when(level >= d)
                def _():
                    pass_on(level - d, side)
                    pass_on(level - d, 1 - side)

                @pl.when(level + d < height)
                def _():
                    pass_on(level + d, side)
                    pass_on(level + d, 1 - side)

                return c

            pass_on(level, 1 - side)
            lax.fori_loop(1, height, near, 0)
            peers(lambda d: to_twin(m, ahead(d), twin_part).wait_recv())
            peers(lambda d: pass_mate(m, ahead(d), twin_mate_part).wait_recv())

    loads[4].wait()
    own_each(0, begin)

    def slot_at(index):
        return pl.ds(pl.multiple_of(index * slots, ROW_TILE), slots)

    def exchange_copy(kind, send, recv, peer, owner):
        return pltpu.make_async_remote_copy(
            src_ref=send.at[slot_at(peer)],
            dst_ref=recv.at[slot_at(owner)],
            send_sem=send_sem.at[SEND_BASE + kind, peer],
            recv_sem=recv_sem.at[RECV_BASE + kind, owner],
            device_id={"ep": peer},
            device_id_type=MESH,
        )

    def own_copy(kind, send, recv):
        return pltpu.make_async_copy(
            send.at[slot_at(me)], recv.at[slot_at(me)], recv_sem.at[RECV_BASE + kind, me]
        )

    def exchange_start(kind, send, recv):
        peers(lambda d: exchange_copy(kind, send, recv, after(d), me).start())
        own_copy(kind, send, recv).start()

    def exchange_wait(kind, send, recv):
        own_copy(kind, send, recv).wait()
        peers(lambda d: exchange_copy(kind, send, recv, after(d), ahead(d)).wait_recv())

    choices = ids_ref.shape[0]

    def as_column(line):
        return jnp.transpose(jnp.broadcast_to(line, (tok_rows, tok_rows)))[:, 0:1]

    ids = [
        as_column(ids_ref[k : k + 1, :].astype(jnp.float32)).astype(jnp.int32)
        for k in range(choices)
    ]
    gates = [as_column(gates_ref[k : k + 1, :]) for k in range(choices)]
    lanes = lax.broadcasted_iota(jnp.int32, (tok_rows, ep_size), 1)
    picks = [(ids[k] == lanes).astype(jnp.float32) for k in range(choices)]
    routed = functools.reduce(jnp.add, picks)
    lower = (
        lax.broadcasted_iota(jnp.int32, (tok_rows, tok_rows), 1)
        < lax.broadcasted_iota(jnp.int32, (tok_rows, tok_rows), 0)
    ).astype(bf16)
    before = dot(lower, routed.astype(bf16))
    by_token = lax.broadcasted_iota(jnp.int32, (tok_rows, total), 1)
    by_slot = lax.broadcasted_iota(jnp.int32, (total, tok_rows), 0)
    take, place = [], []
    for k in range(choices):
        pos = jnp.sum(picks[k] * before, axis=1, keepdims=True)
        flat = ids[k].astype(jnp.float32) * slots + pos
        take.append((flat.astype(jnp.int32) == by_token).astype(bf16))
        flat_row = jnp.transpose(jnp.broadcast_to(flat, (tok_rows, tok_rows)))[0:1, :]
        place.append((flat_row.astype(jnp.int32) == by_slot).astype(bf16))

    loads[5].wait()
    full_up[pl.ds(pl.multiple_of(me * shard, ROW_TILE), shard), :] = jnp.transpose(
        up_shard[...].astype(jnp.float32)
    ).astype(bf16)

    steps(0, 1, 2)
    cross_each(0, 0, begin, arrived)
    own_each(1, begin)
    steps(0, 2, height)
    steps(1, 1, 2)
    cross_each(1, 0, begin, arrived)
    gather_end(0)
    loads[0].wait()
    latent = dot(tokens[...], full_down[...]).astype(bf16)
    lat_send[...] = dot(functools.reduce(jnp.add, place), latent).astype(bf16)
    exchange_start(LATENT, lat_send, lat_recv)

    steps(1, 2, height)
    gather_end(1)
    loads[1].wait()
    grad_latent = dot(grad_out[...], full_up[...])
    sent = [dot(place[k], (gates[k] * grad_latent).astype(bf16)) for k in range(choices)]
    grad_send[...] = functools.reduce(jnp.add, sent).astype(bf16)
    exchange_start(GRAD, grad_send, grad_recv)

    rows = total if total <= 512 else 256
    blocks = total // rows

    def each_block(body):
        if blocks == 1:
            body(slice(None))
        else:
            lax.fori_loop(
                0,
                blocks,
                lambda b, c: (body(pl.ds(pl.multiple_of(b * rows, ROW_TILE), rows)), c)[1],
                0,
            )

    def forward(at):
        hidden = jnp.maximum(dot(lat_recv[at, :], expert_up[...]), 0.0)
        pre_act[at, :] = hidden
        out_send[at, :] = dot((hidden * hidden).astype(bf16), expert_down[...]).astype(bf16)

    loads[2].wait()
    loads[3].wait()
    exchange_wait(LATENT, lat_send, lat_recv)
    each_block(forward)
    exchange_start(FORWARD, out_send, out_recv)

    def backward(at):
        grad_act = contract_last(grad_recv[at, :], expert_down[...])
        grad_pre = (2.0 * pre_act[at, :] * grad_act).astype(bf16)
        in_send[at, :] = contract_last(grad_pre, expert_up[...]).astype(bf16)

    exchange_wait(GRAD, grad_send, grad_recv)
    each_block(backward)
    exchange_start(BACKWARD, in_send, in_recv)

    exchange_wait(FORWARD, out_send, out_recv)
    returned = out_recv[...]
    combined = functools.reduce(
        jnp.add, [gates[k] * dot(take[k], returned) for k in range(choices)]
    ).astype(bf16)
    layer_ref[...] = contract_last(combined, full_up[...]).astype(bf16)

    exchange_wait(BACKWARD, in_send, in_recv)
    grad_sum = dot(functools.reduce(jnp.add, take), in_recv[...]).astype(bf16)
    grad_ref[...] = contract_last(grad_sum, full_down[...]).astype(bf16)

    def finish(d):
        exchange_copy(LATENT, lat_send, lat_recv, after(d), me).wait_send()
        exchange_copy(GRAD, grad_send, grad_recv, after(d), me).wait_send()
        exchange_copy(FORWARD, out_send, out_recv, after(d), me).wait_send()
        exchange_copy(BACKWARD, in_send, in_recv, after(d), me).wait_send()
        if share > 1:
            for m in range(2):
                pass_mate(m, after(d), mate_part).wait_send()

    peers(finish)

    def end(copy):
        copy.wait_send()

    def nothing(m, owner):
        del m, owner

    for m in range(2):
        own_each(m, end)
        cross_each(m, 0, end, nothing)

        def drain(d, c, m=m):
            relay_each(m, d, end, nothing)
            cross_each(m, d, end, nothing)
            return c

        lax.fori_loop(1, height, drain, 0)


def on_device(
    tokens, expert_ids, gate_values, latent_down, latent_up, expert_up, expert_down, grad_out
):
    ep_size = lax.axis_size("ep")
    dp_size = lax.axis_size("dp")
    tok_rows, model = tokens.shape
    top_count = expert_ids.shape[1]
    local_experts, width, hidden = expert_up.shape
    assert local_experts == 1 and ep_size % 2 == 0
    experts = local_experts * ep_size
    capacity = max(2, (3 * tok_rows * top_count + 2 * experts - 1) // (2 * experts))
    slots = (capacity + ROW_TILE - 1) // ROW_TILE * ROW_TILE
    total = experts * slots
    shard = latent_down.shape[0]
    share = 4 if dp_size % 4 == 0 and shard % (4 * ROW_TILE) == 0 else 1
    bf16 = jnp.bfloat16
    buffer = pltpu.VMEM((total, width), bf16)
    vmem = pl.BlockSpec(memory_space=pltpu.VMEM)
    anywhere = pl.BlockSpec(memory_space=pl.ANY)
    return pl.pallas_call(
        functools.partial(kernel, ep_size, share, slots),
        out_shape=[jax.ShapeDtypeStruct((tok_rows, model), bf16)] * 2,
        in_specs=[vmem, vmem] + [anywhere] * 6,
        out_specs=[vmem, vmem],
        scratch_shapes=[
            pltpu.VMEM((tok_rows, model), bf16),
            pltpu.VMEM((tok_rows, model), bf16),
            pltpu.VMEM((width, hidden), bf16),
            pltpu.VMEM((hidden, width), bf16),
            pltpu.VMEM((model, width), bf16),
            pltpu.VMEM((model, width), bf16),
            pltpu.VMEM((width, shard), bf16),
            buffer,
            buffer,
            buffer,
            buffer,
            pltpu.VMEM((total, hidden), jnp.float32),
            buffer,
            buffer,
            buffer,
            buffer,
            pltpu.SemaphoreType.DMA((6,)),
            pltpu.SemaphoreType.DMA((16, ep_size)),
            pltpu.SemaphoreType.DMA((12, ep_size)),
        ],
        compiler_params=pltpu.CompilerParams(
            collective_id=0, has_side_effects=True, vmem_limit_bytes=60 * 1024 * 1024
        ),
    )(
        expert_ids.T,
        gate_values.T,
        tokens,
        grad_out,
        latent_down,
        latent_up,
        expert_up,
        expert_down,
    )


def solution(mesh):
    placed = (
        P(("dp", "ep"), None),
        P(("dp", "ep"), None),
        P(("dp", "ep"), None),
        P("ep", None),
        P(None, "ep"),
        P("ep", None, None),
        P("ep", None, None),
        P(("dp", "ep"), None),
    )
    return jax.shard_map(
        on_device,
        mesh=mesh,
        in_specs=placed,
        out_specs=(P(("dp", "ep"), None), P(("dp", "ep"), None)),
        check_vma=False,
    )
```

```python
import functools

import jax
import jax.numpy as jnp
from jax import lax
from jax.experimental import pallas as pl
from jax.experimental.pallas import tpu as pltpu
from jax.sharding import PartitionSpec as P

MESH = pl.DeviceIdType.MESH
ROW_TILE = 16

UPWARD, DOWNWARD, ACROSS, TWIN, MATE, TWIN_MATE = range(6)
LATENT, GRAD, FORWARD, BACKWARD = range(4)
SEND_BASE, RECV_BASE = 12, 8


def dot(left, right):
    return jnp.dot(left, right, preferred_element_type=jnp.float32)


def contract_last(left, right):
    return lax.dot_general(
        left, right, (((1,), (1,)), ((), ())), preferred_element_type=jnp.float32
    )


def kernel(
    ep_size,
    share,
    slots,
    ids_ref,
    gates_ref,
    tokens_hbm,
    grad_out_hbm,
    down_hbm,
    up_hbm,
    expert_up_hbm,
    expert_down_hbm,
    layer_ref,
    grad_ref,
    tokens,
    grad_out,
    expert_up,
    expert_down,
    full_down,
    full_up,
    up_shard,
    lat_send,
    lat_recv,
    grad_send,
    grad_recv,
    pre_act,
    out_send,
    out_recv,
    in_send,
    in_recv,
    local_sem,
    send_sem,
    recv_sem,
):
    me = lax.axis_index("ep")
    row = lax.axis_index("dp")
    twin = row + 1 - 2 * lax.rem(row, 2)
    mate = row + 2 - 4 * lax.rem(row // 2, 2)
    part, twin_part, mate_part = [
        lax.rem(r, 4) if share > 1 else 0 for r in (row, twin, mate)
    ]
    twin_mate_part = 6 - part - twin_part - mate_part
    shard = down_hbm.shape[0]
    piece = shard // share
    tok_rows = tokens.shape[0]
    total = lat_send.shape[0]
    bf16 = jnp.bfloat16

    def peers(body):
        lax.fori_loop(1, ep_size, lambda d, c: (body(d), c)[1], 0)

    def after(d):
        return lax.rem(me + d, ep_size)

    def ahead(d):
        return lax.rem(me + ep_size - d, ep_size)

    loads = [
        pltpu.make_async_copy(src, dst, local_sem.at[i])
        for i, (src, dst) in enumerate(
            (
                (tokens_hbm, tokens),
                (grad_out_hbm, grad_out),
                (expert_up_hbm.at[0], expert_up),
                (expert_down_hbm.at[0], expert_down),
                (down_hbm, full_down.at[pl.ds(pl.multiple_of(me * shard, ROW_TILE), shard)]),
                (up_hbm, up_shard),
            )
        )
    ]
    for load in loads:
        load.start()

    barrier = pltpu.get_barrier_semaphore()

    def greet(d):
        pl.semaphore_signal(barrier, inc=1, device_id={"ep": after(d)}, device_id_type=MESH)

    peers(greet)
    if share > 1:
        pl.semaphore_signal(barrier, inc=1, device_id={"dp": twin}, device_id_type=MESH)
        pl.semaphore_signal(barrier, inc=1, device_id={"dp": mate}, device_id_type=MESH)
    pl.semaphore_wait(barrier, ep_size - 1 + (2 if share > 1 else 0))

    def piece_at(owner, which):
        return pl.ds(pl.multiple_of(owner * shard + which * piece, ROW_TILE), piece)

    full = (full_down, full_up)
    height = ep_size // 2
    level = me // 2
    side = lax.rem(me, 2)

    def piece_copy(m, owner, which, target, row_of, arrival=0):
        return pltpu.make_async_remote_copy(
            src_ref=full[m].at[piece_at(owner, which)],
            dst_ref=full[m].at[piece_at(owner, which)],
            send_sem=send_sem.at[6 * m + row_of, owner],
            recv_sem=recv_sem.at[4 * m + arrival, owner],
            device_id=target,
            device_id_type=MESH,
        )

    def upward(m, owner):
        return piece_copy(m, owner, part, {"ep": me + 2}, UPWARD)

    def downward(m, owner):
        return piece_copy(m, owner, part, {"ep": me - 2}, DOWNWARD)

    def across(m, owner):
        return piece_copy(m, owner, part, {"ep": me + 1 - 2 * side}, ACROSS)

    def to_twin(m, owner, which):
        return piece_copy(m, owner, which, {"dp": twin}, TWIN, 1)

    def to_mate(m, owner, which):
        return piece_copy(m, owner, which, {"dp": mate}, MATE, 2)

    def pass_mate(m, owner, which):
        return piece_copy(m, owner, which, {"dp": twin}, TWIN_MATE, 3)

    def share_out(m, owner, act):
        if share > 1:
            act(to_mate(m, owner, part))
            act(to_twin(m, owner, part))

    def own_each(m, act):
        @pl.when(level + 1 < height)
        def _():
            act(upward(m, me))

        @pl.when(level > 0)
        def _():
            act(downward(m, me))

        act(across(m, me))

    def relay_each(m, d, act, arrive):
        @pl.when(level >= d)
        def _():
            owner = me - 2 * d
            arrive(m, owner)

            @pl.when(level + 1 < height)
            def _():
                act(upward(m, owner))

            act(across(m, owner))
            share_out(m, owner, act)

        @pl.when(level + d < height)
        def _():
            owner = me + 2 * d
            arrive(m, owner)

            @pl.when(level > 0)
            def _():
                act(downward(m, owner))

            act(across(m, owner))
            share_out(m, owner, act)

    def cross_each(m, d, act, arrive):
        partner = me + 1 - 2 * side

        @pl.when(level >= d)
        def _():
            arrive(m, partner - 2 * d)
            share_out(m, partner - 2 * d, act)

        if not (isinstance(d, int) and d == 0):

            @pl.when(level + d < height)
            def _():
                arrive(m, partner + 2 * d)
                share_out(m, partner + 2 * d, act)

    def begin(copy):
        copy.start()

    def arrived(m, owner):
        across(m, owner).wait_recv()

    def steps(m, first, last):
        def body(d, c):
            relay_each(m, d, begin, arrived)

            @pl.when(d > 1)
            def _():
                cross_each(m, d - 1, begin, arrived)

            return c

        lax.fori_loop(first, last, body, 0)

    def gather_end(m):
        if height > 1:
            cross_each(m, height - 1, begin, arrived)
        if share > 1:

            def pass_on(level_of, side_of):
                owner = level_of * 2 + side_of
                to_mate(m, owner, mate_part).wait_recv()
                pass_mate(m, owner, mate_part).start()

            def near(d, c):
                @pl.when(level >= d)
                def _():
                    pass_on(level - d, side)
                    pass_on(level - d, 1 - side)

                @pl.when(level + d < height)
                def _():
                    pass_on(level + d, side)
                    pass_on(level + d, 1 - side)

                return c

            pass_on(level, 1 - side)
            lax.fori_loop(1, height, near, 0)
            peers(lambda d: to_twin(m, ahead(d), twin_part).wait_recv())
            peers(lambda d: pass_mate(m, ahead(d), twin_mate_part).wait_recv())

    loads[4].wait()
    own_each(0, begin)

    def slot_at(index):
        return pl.ds(pl.multiple_of(index * slots, ROW_TILE), slots)

    def exchange_copy(kind, send, recv, peer, owner):
        return pltpu.make_async_remote_copy(
            src_ref=send.at[slot_at(peer)],
            dst_ref=recv.at[slot_at(owner)],
            send_sem=send_sem.at[SEND_BASE + kind, peer],
            recv_sem=recv_sem.at[RECV_BASE + kind, owner],
            device_id={"ep": peer},
            device_id_type=MESH,
        )

    def own_copy(kind, send, recv):
        return pltpu.make_async_copy(
            send.at[slot_at(me)], recv.at[slot_at(me)], recv_sem.at[RECV_BASE + kind, me]
        )

    half = ep_size // 2
    near_base = me // half * half
    far_base = half - near_base

    def each_near(body):
        lax.fori_loop(
            1, half, lambda i, c: (body(near_base + lax.rem(me + i, half)), c)[1], 0
        )

    def each_far(body):
        lax.fori_loop(
            0, half, lambda i, c: (body(far_base + lax.rem(me + i, half)), c)[1], 0
        )

    def start_near(kind, send, recv):
        each_near(lambda p: exchange_copy(kind, send, recv, p, me).start())
        own_copy(kind, send, recv).start()

    def start_far(kind, send, recv):
        each_far(lambda p: exchange_copy(kind, send, recv, p, me).start())

    def wait_near(kind, send, recv):
        own_copy(kind, send, recv).wait()
        each_near(lambda p: exchange_copy(kind, send, recv, p, p).wait_recv())

    def wait_far(kind, send, recv):
        each_far(lambda p: exchange_copy(kind, send, recv, p, p).wait_recv())

    def exchange_start(kind, send, recv):
        start_far(kind, send, recv)
        start_near(kind, send, recv)

    def exchange_wait(kind, send, recv):
        wait_near(kind, send, recv)
        wait_far(kind, send, recv)

    choices = ids_ref.shape[0]

    def as_column(line):
        return jnp.transpose(jnp.broadcast_to(line, (tok_rows, tok_rows)))[:, 0:1]

    ids = [
        as_column(ids_ref[k : k + 1, :].astype(jnp.float32)).astype(jnp.int32)
        for k in range(choices)
    ]
    gates = [as_column(gates_ref[k : k + 1, :]) for k in range(choices)]
    lanes = lax.broadcasted_iota(jnp.int32, (tok_rows, ep_size), 1)
    picks = [(ids[k] == lanes).astype(jnp.float32) for k in range(choices)]
    routed = functools.reduce(jnp.add, picks)
    lower = (
        lax.broadcasted_iota(jnp.int32, (tok_rows, tok_rows), 1)
        < lax.broadcasted_iota(jnp.int32, (tok_rows, tok_rows), 0)
    ).astype(bf16)
    before = dot(lower, routed.astype(bf16))
    by_token = lax.broadcasted_iota(jnp.int32, (tok_rows, total), 1)
    by_slot = lax.broadcasted_iota(jnp.int32, (total, tok_rows), 0)
    take, place = [], []
    for k in range(choices):
        pos = jnp.sum(picks[k] * before, axis=1, keepdims=True)
        flat = ids[k].astype(jnp.float32) * slots + pos
        take.append((flat.astype(jnp.int32) == by_token).astype(bf16))
        flat_row = jnp.transpose(jnp.broadcast_to(flat, (tok_rows, tok_rows)))[0:1, :]
        place.append((flat_row.astype(jnp.int32) == by_slot).astype(bf16))

    loads[5].wait()
    full_up[pl.ds(pl.multiple_of(me * shard, ROW_TILE), shard), :] = jnp.transpose(
        up_shard[...].astype(jnp.float32)
    ).astype(bf16)

    steps(0, 1, 2)
    cross_each(0, 0, begin, arrived)
    own_each(1, begin)
    steps(0, 2, height)
    steps(1, 1, 2)
    cross_each(1, 0, begin, arrived)
    gather_end(0)
    loads[0].wait()
    latent = dot(tokens[...], full_down[...]).astype(bf16)
    lat_send[...] = dot(functools.reduce(jnp.add, place), latent).astype(bf16)
    exchange_start(LATENT, lat_send, lat_recv)

    steps(1, 2, height)
    gather_end(1)
    loads[1].wait()
    grad_latent = dot(grad_out[...], full_up[...])
    sent = [dot(place[k], (gates[k] * grad_latent).astype(bf16)) for k in range(choices)]
    grad_send[...] = functools.reduce(jnp.add, sent).astype(bf16)
    exchange_start(GRAD, grad_send, grad_recv)

    rows = half * slots if half * slots <= 512 else 256

    def each_block(base, body):
        lax.fori_loop(
            0,
            half * slots // rows,
            lambda b, c: (
                body(pl.ds(pl.multiple_of(base * slots + b * rows, ROW_TILE), rows)),
                c,
            )[1],
            0,
        )

    def forward(at):
        hidden = jnp.maximum(dot(lat_recv[at, :], expert_up[...]), 0.0)
        pre_act[at, :] = hidden
        out_send[at, :] = dot((hidden * hidden).astype(bf16), expert_down[...]).astype(bf16)

    loads[2].wait()
    loads[3].wait()
    wait_near(LATENT, lat_send, lat_recv)
    each_block(near_base, forward)
    start_near(FORWARD, out_send, out_recv)
    wait_far(LATENT, lat_send, lat_recv)
    each_block(far_base, forward)
    start_far(FORWARD, out_send, out_recv)

    def backward(at):
        grad_act = contract_last(grad_recv[at, :], expert_down[...])
        grad_pre = (2.0 * pre_act[at, :] * grad_act).astype(bf16)
        in_send[at, :] = contract_last(grad_pre, expert_up[...]).astype(bf16)

    wait_near(GRAD, grad_send, grad_recv)
    each_block(near_base, backward)
    start_near(BACKWARD, in_send, in_recv)
    wait_far(GRAD, grad_send, grad_recv)
    each_block(far_base, backward)
    start_far(BACKWARD, in_send, in_recv)

    exchange_wait(FORWARD, out_send, out_recv)
    returned = out_recv[...]
    combined = functools.reduce(
        jnp.add, [gates[k] * dot(take[k], returned) for k in range(choices)]
    ).astype(bf16)
    layer_ref[...] = contract_last(combined, full_up[...]).astype(bf16)

    exchange_wait(BACKWARD, in_send, in_recv)
    grad_sum = dot(functools.reduce(jnp.add, take), in_recv[...]).astype(bf16)
    grad_ref[...] = contract_last(grad_sum, full_down[...]).astype(bf16)

    def finish(d):
        exchange_copy(LATENT, lat_send, lat_recv, after(d), me).wait_send()
        exchange_copy(GRAD, grad_send, grad_recv, after(d), me).wait_send()
        exchange_copy(FORWARD, out_send, out_recv, after(d), me).wait_send()
        exchange_copy(BACKWARD, in_send, in_recv, after(d), me).wait_send()
        if share > 1:
            for m in range(2):
                pass_mate(m, after(d), mate_part).wait_send()

    peers(finish)

    def end(copy):
        copy.wait_send()

    def nothing(m, owner):
        del m, owner

    for m in range(2):
        own_each(m, end)
        cross_each(m, 0, end, nothing)

        def drain(d, c, m=m):
            relay_each(m, d, end, nothing)
            cross_each(m, d, end, nothing)
            return c

        lax.fori_loop(1, height, drain, 0)


def on_device(
    tokens, expert_ids, gate_values, latent_down, latent_up, expert_up, expert_down, grad_out
):
    ep_size = lax.axis_size("ep")
    dp_size = lax.axis_size("dp")
    tok_rows, model = tokens.shape
    top_count = expert_ids.shape[1]
    local_experts, width, hidden = expert_up.shape
    assert local_experts == 1 and ep_size % 2 == 0
    experts = local_experts * ep_size
    capacity = max(2, (3 * tok_rows * top_count + 2 * experts - 1) // (2 * experts))
    slots = (capacity + ROW_TILE - 1) // ROW_TILE * ROW_TILE
    total = experts * slots
    shard = latent_down.shape[0]
    share = 4 if dp_size % 4 == 0 and shard % (4 * ROW_TILE) == 0 else 1
    bf16 = jnp.bfloat16
    buffer = pltpu.VMEM((total, width), bf16)
    vmem = pl.BlockSpec(memory_space=pltpu.VMEM)
    anywhere = pl.BlockSpec(memory_space=pl.ANY)
    return pl.pallas_call(
        functools.partial(kernel, ep_size, share, slots),
        out_shape=[jax.ShapeDtypeStruct((tok_rows, model), bf16)] * 2,
        in_specs=[vmem, vmem] + [anywhere] * 6,
        out_specs=[vmem, vmem],
        scratch_shapes=[
            pltpu.VMEM((tok_rows, model), bf16),
            pltpu.VMEM((tok_rows, model), bf16),
            pltpu.VMEM((width, hidden), bf16),
            pltpu.VMEM((hidden, width), bf16),
            pltpu.VMEM((model, width), bf16),
            pltpu.VMEM((model, width), bf16),
            pltpu.VMEM((width, shard), bf16),
            buffer,
            buffer,
            buffer,
            buffer,
            pltpu.VMEM((total, hidden), jnp.float32),
            buffer,
            buffer,
            buffer,
            buffer,
            pltpu.SemaphoreType.DMA((6,)),
            pltpu.SemaphoreType.DMA((16, ep_size)),
            pltpu.SemaphoreType.DMA((12, ep_size)),
        ],
        compiler_params=pltpu.CompilerParams(
            collective_id=0, has_side_effects=True, vmem_limit_bytes=60 * 1024 * 1024
        ),
    )(
        expert_ids.T,
        gate_values.T,
        tokens,
        grad_out,
        latent_down,
        latent_up,
        expert_up,
        expert_down,
    )


def solution(mesh):
    placed = (
        P(("dp", "ep"), None),
        P(("dp", "ep"), None),
        P(("dp", "ep"), None),
        P("ep", None),
        P(None, "ep"),
        P("ep", None, None),
        P("ep", None, None),
        P(("dp", "ep"), None),
    )
    return jax.shard_map(
        on_device,
        mesh=mesh,
        in_specs=placed,
        out_specs=(P(("dp", "ep"), None), P(("dp", "ep"), None)),
        check_vma=False,
    )
```

```python
import functools

import jax
import jax.numpy as jnp
from jax import lax
from jax.experimental import pallas as pl
from jax.experimental.pallas import tpu as pltpu
from jax.sharding import PartitionSpec as P

MESH = pl.DeviceIdType.MESH
ROW_TILE = 16

UPWARD, DOWNWARD, ACROSS, TWIN, MATE, TWIN_MATE = range(6)
LATENT, GRAD, FORWARD, BACKWARD = range(4)
SEND_BASE, RECV_BASE = 12, 8


def dot(left, right):
    return jnp.dot(left, right, preferred_element_type=jnp.float32)


def contract_last(left, right):
    return lax.dot_general(
        left, right, (((1,), (1,)), ((), ())), preferred_element_type=jnp.float32
    )


def kernel(
    ep_size,
    share,
    slots,
    ids_ref,
    gates_ref,
    tokens_hbm,
    grad_out_hbm,
    down_hbm,
    up_hbm,
    expert_up_hbm,
    expert_down_hbm,
    layer_ref,
    grad_ref,
    tokens,
    grad_out,
    expert_up,
    expert_down,
    full_down,
    full_up,
    up_shard,
    lat_send,
    lat_recv,
    grad_send,
    grad_recv,
    pre_act,
    out_send,
    out_recv,
    in_send,
    in_recv,
    local_sem,
    send_sem,
    recv_sem,
):
    me = lax.axis_index("ep")
    row = lax.axis_index("dp")
    twin = row + 1 - 2 * lax.rem(row, 2)
    mate = row + 2 - 4 * lax.rem(row // 2, 2)
    part, twin_part, mate_part = [
        lax.rem(r, 4) if share > 1 else 0 for r in (row, twin, mate)
    ]
    twin_mate_part = 6 - part - twin_part - mate_part
    shard = down_hbm.shape[0]
    piece = shard // share
    tok_rows = tokens.shape[0]
    total = lat_send.shape[0]
    bf16 = jnp.bfloat16

    def peers(body):
        lax.fori_loop(1, ep_size, lambda d, c: (body(d), c)[1], 0)

    def after(d):
        return lax.rem(me + d, ep_size)

    def ahead(d):
        return lax.rem(me + ep_size - d, ep_size)

    loads = [
        pltpu.make_async_copy(src, dst, local_sem.at[i])
        for i, (src, dst) in enumerate(
            (
                (tokens_hbm, tokens),
                (grad_out_hbm, grad_out),
                (expert_up_hbm.at[0], expert_up),
                (expert_down_hbm.at[0], expert_down),
                (down_hbm, full_down.at[pl.ds(pl.multiple_of(me * shard, ROW_TILE), shard)]),
                (up_hbm, up_shard),
            )
        )
    ]
    for load in loads:
        load.start()

    barrier = pltpu.get_barrier_semaphore()

    def greet(d):
        pl.semaphore_signal(barrier, inc=1, device_id={"ep": after(d)}, device_id_type=MESH)

    peers(greet)
    if share > 1:
        pl.semaphore_signal(barrier, inc=1, device_id={"dp": twin}, device_id_type=MESH)
        pl.semaphore_signal(barrier, inc=1, device_id={"dp": mate}, device_id_type=MESH)
    pl.semaphore_wait(barrier, ep_size - 1 + (2 if share > 1 else 0))

    def piece_at(owner, which):
        return pl.ds(pl.multiple_of(owner * shard + which * piece, ROW_TILE), piece)

    full = (full_down, full_up)
    height = ep_size // 2
    level = me // 2
    side = lax.rem(me, 2)

    def piece_copy(m, owner, which, target, row_of, arrival=0):
        return pltpu.make_async_remote_copy(
            src_ref=full[m].at[piece_at(owner, which)],
            dst_ref=full[m].at[piece_at(owner, which)],
            send_sem=send_sem.at[6 * m + row_of, owner],
            recv_sem=recv_sem.at[4 * m + arrival, owner],
            device_id=target,
            device_id_type=MESH,
        )

    def upward(m, owner):
        return piece_copy(m, owner, part, {"ep": me + 2}, UPWARD)

    def downward(m, owner):
        return piece_copy(m, owner, part, {"ep": me - 2}, DOWNWARD)

    def across(m, owner):
        return piece_copy(m, owner, part, {"ep": me + 1 - 2 * side}, ACROSS)

    def to_twin(m, owner, which):
        return piece_copy(m, owner, which, {"dp": twin}, TWIN, 1)

    def to_mate(m, owner, which):
        return piece_copy(m, owner, which, {"dp": mate}, MATE, 2)

    def pass_mate(m, owner, which):
        return piece_copy(m, owner, which, {"dp": twin}, TWIN_MATE, 3)

    def share_out(m, owner, act):
        if share > 1:
            act(to_mate(m, owner, part))
            act(to_twin(m, owner, part))

    def own_each(m, act):
        @pl.when(level + 1 < height)
        def _():
            act(upward(m, me))

        @pl.when(level > 0)
        def _():
            act(downward(m, me))

        act(across(m, me))

    def relay_each(m, d, act, arrive):
        @pl.when(level >= d)
        def _():
            owner = me - 2 * d
            arrive(m, owner)

            @pl.when(level + 1 < height)
            def _():
                act(upward(m, owner))

            act(across(m, owner))
            share_out(m, owner, act)

        @pl.when(level + d < height)
        def _():
            owner = me + 2 * d
            arrive(m, owner)

            @pl.when(level > 0)
            def _():
                act(downward(m, owner))

            act(across(m, owner))
            share_out(m, owner, act)

    def cross_each(m, d, act, arrive):
        partner = me + 1 - 2 * side

        @pl.when(level >= d)
        def _():
            arrive(m, partner - 2 * d)
            share_out(m, partner - 2 * d, act)

        if not (isinstance(d, int) and d == 0):

            @pl.when(level + d < height)
            def _():
                arrive(m, partner + 2 * d)
                share_out(m, partner + 2 * d, act)

    def begin(copy):
        copy.start()

    def arrived(m, owner):
        across(m, owner).wait_recv()

    def steps(m, first, last):
        def body(d, c):
            relay_each(m, d, begin, arrived)

            @pl.when(d > 1)
            def _():
                cross_each(m, d - 1, begin, arrived)

            return c

        lax.fori_loop(first, last, body, 0)

    def gather_end(m):
        if height > 1:
            cross_each(m, height - 1, begin, arrived)
        if share > 1:

            def pass_on(level_of, side_of):
                owner = level_of * 2 + side_of
                to_mate(m, owner, mate_part).wait_recv()
                pass_mate(m, owner, mate_part).start()

            def near(d, c):
                @pl.when(level >= d)
                def _():
                    pass_on(level - d, side)
                    pass_on(level - d, 1 - side)

                @pl.when(level + d < height)
                def _():
                    pass_on(level + d, side)
                    pass_on(level + d, 1 - side)

                return c

            pass_on(level, 1 - side)
            lax.fori_loop(1, height, near, 0)
            peers(lambda d: to_twin(m, ahead(d), twin_part).wait_recv())
            peers(lambda d: pass_mate(m, ahead(d), twin_mate_part).wait_recv())

    loads[4].wait()
    own_each(0, begin)

    def slot_at(index):
        return pl.ds(pl.multiple_of(index * slots, ROW_TILE), slots)

    def exchange_copy(kind, send, recv, peer, owner):
        return pltpu.make_async_remote_copy(
            src_ref=send.at[slot_at(peer)],
            dst_ref=recv.at[slot_at(owner)],
            send_sem=send_sem.at[SEND_BASE + kind, peer],
            recv_sem=recv_sem.at[RECV_BASE + kind, owner],
            device_id={"ep": peer},
            device_id_type=MESH,
        )

    def own_copy(kind, send, recv):
        return pltpu.make_async_copy(
            send.at[slot_at(me)], recv.at[slot_at(me)], recv_sem.at[RECV_BASE + kind, me]
        )

    def exchange_start(kind, send, recv):
        peers(lambda d: exchange_copy(kind, send, recv, after(d), me).start())
        own_copy(kind, send, recv).start()

    def exchange_wait(kind, send, recv):
        own_copy(kind, send, recv).wait()
        peers(lambda d: exchange_copy(kind, send, recv, after(d), ahead(d)).wait_recv())

    choices = ids_ref.shape[0]

    def as_column(line):
        return jnp.transpose(jnp.broadcast_to(line, (tok_rows, tok_rows)))[:, 0:1]

    ids = [
        as_column(ids_ref[k : k + 1, :].astype(jnp.float32)).astype(jnp.int32)
        for k in range(choices)
    ]
    gates = [as_column(gates_ref[k : k + 1, :]) for k in range(choices)]
    lanes = lax.broadcasted_iota(jnp.int32, (tok_rows, ep_size), 1)
    picks = [(ids[k] == lanes).astype(jnp.float32) for k in range(choices)]
    routed = functools.reduce(jnp.add, picks)
    lower = (
        lax.broadcasted_iota(jnp.int32, (tok_rows, tok_rows), 1)
        < lax.broadcasted_iota(jnp.int32, (tok_rows, tok_rows), 0)
    ).astype(bf16)
    before = dot(lower, routed.astype(bf16))
    by_token = lax.broadcasted_iota(jnp.int32, (tok_rows, total), 1)
    by_slot = lax.broadcasted_iota(jnp.int32, (total, tok_rows), 0)
    take, place = [], []
    for k in range(choices):
        pos = jnp.sum(picks[k] * before, axis=1, keepdims=True)
        flat = ids[k].astype(jnp.float32) * slots + pos
        take.append((flat.astype(jnp.int32) == by_token).astype(bf16))
        flat_row = jnp.transpose(jnp.broadcast_to(flat, (tok_rows, tok_rows)))[0:1, :]
        place.append((flat_row.astype(jnp.int32) == by_slot).astype(bf16))

    loads[5].wait()
    full_up[pl.ds(pl.multiple_of(me * shard, ROW_TILE), shard), :] = jnp.transpose(
        up_shard[...].astype(jnp.float32)
    ).astype(bf16)

    steps(0, 1, 2)
    cross_each(0, 0, begin, arrived)
    own_each(1, begin)
    steps(0, 2, height)
    steps(1, 1, 2)
    cross_each(1, 0, begin, arrived)
    gather_end(0)
    loads[0].wait()
    latent = dot(tokens[...], full_down[...]).astype(bf16)
    lat_send[...] = dot(functools.reduce(jnp.add, place), latent).astype(bf16)
    exchange_start(LATENT, lat_send, lat_recv)

    steps(1, 2, height)

    rows = total if total <= 512 else 256
    blocks = total // rows

    def each_block(body):
        if blocks == 1:
            body(slice(None))
        else:
            lax.fori_loop(
                0,
                blocks,
                lambda b, c: (body(pl.ds(pl.multiple_of(b * rows, ROW_TILE), rows)), c)[1],
                0,
            )

    def forward(at):
        hidden = jnp.maximum(dot(lat_recv[at, :], expert_up[...]), 0.0)
        pre_act[at, :] = hidden
        out_send[at, :] = dot((hidden * hidden).astype(bf16), expert_down[...]).astype(bf16)

    loads[2].wait()
    loads[3].wait()
    exchange_wait(LATENT, lat_send, lat_recv)
    each_block(forward)
    exchange_start(FORWARD, out_send, out_recv)

    gather_end(1)
    loads[1].wait()
    grad_latent = dot(grad_out[...], full_up[...])
    sent = [dot(place[k], (gates[k] * grad_latent).astype(bf16)) for k in range(choices)]
    grad_send[...] = functools.reduce(jnp.add, sent).astype(bf16)
    exchange_start(GRAD, grad_send, grad_recv)

    def backward(at):
        grad_act = contract_last(grad_recv[at, :], expert_down[...])
        grad_pre = (2.0 * pre_act[at, :] * grad_act).astype(bf16)
        in_send[at, :] = contract_last(grad_pre, expert_up[...]).astype(bf16)

    exchange_wait(GRAD, grad_send, grad_recv)
    each_block(backward)
    exchange_start(BACKWARD, in_send, in_recv)

    exchange_wait(FORWARD, out_send, out_recv)
    returned = out_recv[...]
    combined = functools.reduce(
        jnp.add, [gates[k] * dot(take[k], returned) for k in range(choices)]
    ).astype(bf16)
    layer_ref[...] = contract_last(combined, full_up[...]).astype(bf16)

    exchange_wait(BACKWARD, in_send, in_recv)
    grad_sum = dot(functools.reduce(jnp.add, take), in_recv[...]).astype(bf16)
    grad_ref[...] = contract_last(grad_sum, full_down[...]).astype(bf16)

    def finish(d):
        exchange_copy(LATENT, lat_send, lat_recv, after(d), me).wait_send()
        exchange_copy(GRAD, grad_send, grad_recv, after(d), me).wait_send()
        exchange_copy(FORWARD, out_send, out_recv, after(d), me).wait_send()
        exchange_copy(BACKWARD, in_send, in_recv, after(d), me).wait_send()
        if share > 1:
            for m in range(2):
                pass_mate(m, after(d), mate_part).wait_send()

    peers(finish)

    def end(copy):
        copy.wait_send()

    def nothing(m, owner):
        del m, owner

    for m in range(2):
        own_each(m, end)
        cross_each(m, 0, end, nothing)

        def drain(d, c, m=m):
            relay_each(m, d, end, nothing)
            cross_each(m, d, end, nothing)
            return c

        lax.fori_loop(1, height, drain, 0)


def on_device(
    tokens, expert_ids, gate_values, latent_down, latent_up, expert_up, expert_down, grad_out
):
    ep_size = lax.axis_size("ep")
    dp_size = lax.axis_size("dp")
    tok_rows, model = tokens.shape
    top_count = expert_ids.shape[1]
    local_experts, width, hidden = expert_up.shape
    assert local_experts == 1 and ep_size % 2 == 0
    experts = local_experts * ep_size
    capacity = max(2, (3 * tok_rows * top_count + 2 * experts - 1) // (2 * experts))
    slots = (capacity + ROW_TILE - 1) // ROW_TILE * ROW_TILE
    total = experts * slots
    shard = latent_down.shape[0]
    share = 4 if dp_size % 4 == 0 and shard % (4 * ROW_TILE) == 0 else 1
    bf16 = jnp.bfloat16
    buffer = pltpu.VMEM((total, width), bf16)
    vmem = pl.BlockSpec(memory_space=pltpu.VMEM)
    anywhere = pl.BlockSpec(memory_space=pl.ANY)
    return pl.pallas_call(
        functools.partial(kernel, ep_size, share, slots),
        out_shape=[jax.ShapeDtypeStruct((tok_rows, model), bf16)] * 2,
        in_specs=[vmem, vmem] + [anywhere] * 6,
        out_specs=[vmem, vmem],
        scratch_shapes=[
            pltpu.VMEM((tok_rows, model), bf16),
            pltpu.VMEM((tok_rows, model), bf16),
            pltpu.VMEM((width, hidden), bf16),
            pltpu.VMEM((hidden, width), bf16),
            pltpu.VMEM((model, width), bf16),
            pltpu.VMEM((model, width), bf16),
            pltpu.VMEM((width, shard), bf16),
            buffer,
            buffer,
            buffer,
            buffer,
            pltpu.VMEM((total, hidden), jnp.float32),
            buffer,
            buffer,
            buffer,
            buffer,
            pltpu.SemaphoreType.DMA((6,)),
            pltpu.SemaphoreType.DMA((16, ep_size)),
            pltpu.SemaphoreType.DMA((12, ep_size)),
        ],
        compiler_params=pltpu.CompilerParams(
            collective_id=0, has_side_effects=True, vmem_limit_bytes=60 * 1024 * 1024
        ),
    )(
        expert_ids.T,
        gate_values.T,
        tokens,
        grad_out,
        latent_down,
        latent_up,
        expert_up,
        expert_down,
    )


def solution(mesh):
    placed = (
        P(("dp", "ep"), None),
        P(("dp", "ep"), None),
        P(("dp", "ep"), None),
        P("ep", None),
        P(None, "ep"),
        P("ep", None, None),
        P("ep", None, None),
        P(("dp", "ep"), None),
    )
    return jax.shard_map(
        on_device,
        mesh=mesh,
        in_specs=placed,
        out_specs=(P(("dp", "ep"), None), P(("dp", "ep"), None)),
        check_vma=False,
    )
```
